128 devices in a mesh: ga: 16 (over x, z_hi, core), ba: 8 (over y, z_lo).
Axes of the slice: x: 4, y: 4, z: 4 (z_hi: 2, z_lo: 2; z = z_hi * 2 + z_lo), core: 2. Of those that a mesh axis runs over, the one named last changes fastest.
Arguments:
- psi: float32 [2, 32768, 2048], P(None, 'ga', 'ba'), may hold values from -0.15625 to 0.15625
- dpsi: float32 [2, 32768, 512], P(None, 'ga', 'ba'), may hold values from -6 to 6
- band_weight: float32 [2048], replicated, may hold values from 0.25 to 1
- panel_band: int32 [16], P('ba'), may hold values from 0 to 15, each once
- slab_offset: int32 [16], replicated, may hold values from 0 to 2047
Outputs:
- projected: float32 [2, 32768, 512], P(None, 'ga', 'ba')
The draws below stay inside these ranges and needn't reach their ends.
Inputs may be any that keep to these rules, and one draw needn't show every extreme that they name: panel_band is a permutation of the panel numbers.
All inputs are finite; a program needn't handle non-finite values.
Results may differ from the reference program's by a relative error of at most 0.00012.
Values sent between devices are 32-bit elements; how exact they have to be, the bound alone decides.
No kernel may reach another device: no remote copies, remote signals or barrier semaphores. Data moves between devices by JAX's collectives and lax.ppermute only.
A program may use at most 128 MiB of HBM per device.

```python
import math
import jax
import jax.numpy as jnp
from jax import lax

NB = 2048
NP = 512
PANEL = 128
NPW_DEV = 2048
NPW = 32768
NPANEL = 16
N_GA = 16


def place_ends(array, rng, low, high):
    place = [jax.random.randint(jax.random.fold_in(rng, axis), (), 0, length) for axis, length in enumerate(array.shape)]
    widest = array.shape.index(max(array.shape))
    neighbour = place[:widest] + [(place[widest] + 1) % array.shape[widest]] + place[widest + 1:]
    return array.at[tuple(place)].set(low).at[tuple(neighbour)].set(high)


def block_scale(rng, shape, shards, least, top_value):
    def one(position, shards_of):
        steps = jax.random.uniform(jax.random.fold_in(jax.random.fold_in(rng, 6), position), (shards_of,), jnp.float32, least / len(shards), top_value / len(shards))
        return jnp.repeat(jnp.exp(steps), shape[position] // shards_of).reshape((-1,) + (1,) * (len(shape) - position - 1))

    factor_of = one(*shards[0])
    for cut in shards[1:]:
        factor_of = factor_of * one(*cut)
    return factor_of


def scatter_about(key, extent, deviation, reach, shards=(), held_as=jnp.bfloat16):
    drawn = jax.random.normal(key, extent, jnp.float32) * deviation
    if len(shards) > 0:
        drawn = block_scale(key, extent, shards, -0.22, 0.18) * drawn
    return jnp.clip(drawn, min=-reach, max=reach).astype(held_as)


def setup_inputs(seed: int = 0) -> dict:
    seeds = jax.random.split(jax.random.key(seed), 6)
    return {
        "psi": scatter_about(seeds[0], (2, NPW, NB), ((NPW * NB) ** -0.25), 0.15625, ((1, 16), (2, 8)), jnp.float32),
        "dpsi": scatter_about(seeds[1], (2, NPW, NP), 1.0, 6.0, ((1, 16), (2, 8)), jnp.float32),
        "band_weight": jnp.clip(jnp.exp(jax.random.uniform(seeds[2], (NB,), jnp.float32, math.log(0.25), math.log(1.0))), 0.25, 1.0),
        "panel_band": jax.random.permutation(seeds[3], NPANEL).astype(jnp.int32),
        "slab_offset": place_ends(jax.random.randint(seeds[4], (N_GA,), 0, NPW_DEV), jax.random.fold_in(seeds[4], 1), 0, NPW_DEV - 1).astype(jnp.int32),
    }


def tdot(left, right):
    return lax.dot_general(left, right, (((0,), (0,)), ((), ())), precision=lax.Precision.HIGHEST, preferred_element_type=jnp.float32)


def mdot(left, right):
    return jnp.dot(left, right, precision=lax.Precision.HIGHEST, preferred_element_type=jnp.float32)


def reference(psi, dpsi, band_weight, panel_band, slab_offset):
    stacked = dpsi.reshape(2, N_GA, NPW_DEV, NP)
    rows = (jnp.arange(NPW_DEV, dtype=jnp.int32)[None, :] + slab_offset[:, None]) % NPW_DEV
    aligned = jnp.take_along_axis(stacked, rows[None, :, :, None], axis=2).reshape(2, NPW, NP)
    weight = band_weight.reshape(NPANEL, PANEL)[panel_band].reshape(NB)
    over_re = tdot(psi[0], aligned[0]) + tdot(psi[1], aligned[1])
    over_im = tdot(psi[0], aligned[1]) - tdot(psi[1], aligned[0])
    w_re = over_re * weight[:, None]
    w_im = over_im * weight[:, None]
    corr_re = mdot(psi[0], w_re) - mdot(psi[1], w_im)
    corr_im = mdot(psi[0], w_im) + mdot(psi[1], w_re)
    diff = (aligned - jnp.stack([corr_re, corr_im])).reshape(2, N_GA, NPW_DEV, NP)
    back = (jnp.arange(NPW_DEV, dtype=jnp.int32)[None, :] - slab_offset[:, None]) % NPW_DEV
    result = jnp.take_along_axis(diff, back[None, :, :, None], axis=2)
    return result.reshape(2, NPW, NP)
```

```python
import jax
import jax.numpy as jnp
from jax import lax
from jax.sharding import Mesh
from jax.sharding import PartitionSpec as P

PANEL = 128
AXES = ("x", "zh", "c", "y", "zl")


def shifted(value, axis, step):
    n = lax.axis_size(axis)
    return lax.ppermute(value, axis, [(i, (i + step) % n) for i in range(n)])


def everyone(value, axes):
    n = lax.axis_size(axes)
    return lax.all_to_all(jnp.broadcast_to(value[None], (n, *value.shape)), axes, 0, 0, tiled=True)


def tdot(left, right):
    return lax.dot_general(
        left,
        right,
        (((0,), (0,)), ((), ())),
        precision=lax.Precision.HIGH,
        preferred_element_type=jnp.float32,
    )


def mdot(left, right):
    return jnp.dot(left, right, precision=lax.Precision.HIGH, preferred_element_type=jnp.float32)


def quarter(value):
    v = value.reshape(*value.shape[:-1], -1, 2, 64)
    return jnp.stack([v[..., 1, :], -v[..., 0, :]], axis=-2).reshape(value.shape)


def gather_y(block):
    half = block.shape[0] // 2
    before = shifted(block, "y", 1)
    after = shifted(block, "y", -1)
    far_a = shifted(before[:half], "y", 1)
    far_b = shifted(after[half:], "y", -1)
    return [block, after, jnp.concatenate([far_a, far_b], 0), before]


def scatter_y(parts):
    half = parts[2].shape[0] // 2
    up = shifted(parts[2][:half], "y", 1)
    down = shifted(parts[2][half:], "y", -1)
    to_next = jnp.concatenate([parts[1][:half] + up, parts[1][half:]], 0)
    to_prev = jnp.concatenate([parts[3][:half], parts[3][half:] + down], 0)
    return parts[0] + (shifted(to_next, "y", 1) + shifted(to_prev, "y", -1))


def per_device(psi, dpsi, band_weight, panel_band, slab_offset):
    ga = lax.axis_index(("x", "zh", "c"))
    zl = lax.axis_index("zl")
    rows = psi.shape[1]
    half = rows // 2
    nb = psi.shape[2]
    np_dev = dpsi.shape[2]
    offset = slab_offset[ga]
    both = jnp.concatenate([dpsi[0], dpsi[1]], axis=1)
    twice = jnp.concatenate([both, both], axis=0)
    mine = lax.dynamic_slice_in_dim(twice, (offset + zl * half) % rows, half, 0)
    other = lax.dynamic_slice_in_dim(twice, (offset + (1 - zl) * half) % rows, half, 0)
    pair = shifted(other, "zl", 1)
    psi_mine = lax.dynamic_slice_in_dim(psi, zl * half, half, 1)
    psi_other = lax.dynamic_slice_in_dim(psi, (1 - zl) * half, half, 1)
    psi_pair = shifted(psi_other, "zl", 1)
    columns = jnp.concatenate(gather_y(mine) + gather_y(pair), axis=1)
    stacked = jnp.concatenate([columns, quarter(columns)], axis=0)
    margin = jnp.stack(
        [tdot(p.reshape(2 * half, nb), stacked) for p in (psi_mine, psi_pair)]
    )
    width = margin.shape[2]
    margin = margin.reshape(2, 2, nb // 2, 2, width // 2)
    margin = jnp.where(zl == 0, margin, jnp.flip(margin, (0, 3)))
    margin = margin.swapaxes(0, 1)
    over_c = lax.all_to_all(margin, "c", 0, 0, tiled=True).sum(0)
    groups = lax.axis_size(("zl", "x", "zh"))
    over_c = over_c.reshape(groups, -1, width)
    total = lax.all_to_all(over_c, ("zl", "x", "zh"), 0, 0, tiled=True).sum(0)
    each = total.shape[0]
    place = (lax.axis_index("c") * (groups // 2) + lax.axis_index(("x", "zh"))) * each
    start = panel_band[place // PANEL] * PANEL + place % PANEL
    weighted = total * lax.dynamic_slice_in_dim(band_weight, start, each)[:, None]
    spread = everyone(weighted, ("zl", "x", "zh")).reshape(2, nb // 2, width)
    spread = everyone(spread, "c").swapaxes(0, 1).reshape(2, nb, 2, width // 2)
    spread = jnp.where(zl == 0, spread, jnp.flip(spread, (0, 2))).reshape(2, nb, width)
    turned = -quarter(spread)
    corr = (
        mdot(psi_mine[0], spread[0])
        + mdot(psi_mine[1], turned[0])
        + mdot(psi_pair[0], spread[1])
        + mdot(psi_pair[1], turned[1])
    )
    lanes = 2 * np_dev
    parts = [corr[:, k * lanes : (k + 1) * lanes] for k in range(width // lanes)]
    away = shifted(scatter_y(parts[4:]), "zl", 1)
    home = scatter_y(parts[:4])
    ring = jnp.concatenate([home, away, home, away], axis=0)
    back = lax.dynamic_slice_in_dim(ring, (2 * rows - offset - zl * half) % rows, rows, 0)
    return dpsi - jnp.stack([back[:, :np_dev], back[:, np_dev:]])


def solution(mesh):
    fine = Mesh(mesh.devices.reshape(4, 2, 2, 4, 2), AXES)
    ga, ba = ("x", "zh", "c"), ("y", "zl")
    in_specs = (P(None, ga, ba), P(None, ga, ba), P(), P(ba), P())
    out_specs = P(None, ga, ba)
    return jax.shard_map(
        per_device, mesh=fine, in_specs=in_specs, out_specs=out_specs, check_vma=False
    )
```

```python
import jax
import jax.numpy as jnp
from jax import lax
from jax.experimental import pallas as pl
from jax.experimental.pallas import tpu as pltpu
from jax.sharding import Mesh
from jax.sharding import PartitionSpec as P


PANEL = 128
AXES = ("x", "zh", "c", "y", "zl")
SPREAD = ("zl", "x", "zh")


def shifted(value, axis, step):
    n = lax.axis_size(axis)
    return lax.ppermute(value, axis, [(i, (i + step) % n) for i in range(n)])


def everyone(value, axes):
    n = lax.axis_size(axes)
    return lax.all_to_all(jnp.broadcast_to(value[None], (n, *value.shape)), axes, 0, 0, tiled=True)


def split(value):
    high = value.astype(jnp.bfloat16)
    low = (value - high.astype(jnp.float32)).astype(jnp.bfloat16)
    return high, low


def dot3(left, right, dims):
    (lh, ll), (rh, rl) = split(left), split(right)

    def dot(a, b):
        return lax.dot_general(a, b, (dims, ((), ())), preferred_element_type=jnp.float32)

    return dot(lh, rh) + (dot(lh, rl) + dot(ll, rh))


def turned(value, block):
    half = block // 2
    pieces = []
    for k in range(0, value.shape[0], block):
        pieces += [value[k + half : k + block], -value[k : k + half]]
    return jnp.concatenate(pieces, axis=0)


def roll_kernel(place, stored, mine, other):
    rows = stored.shape[1]
    lined = pltpu.roll(stored[...], place[2], 1)
    mine[...] = lined[:, : rows // 2]
    other[...] = lined[:, rows // 2 :]


def roll_out(place, stored):
    half = jax.ShapeDtypeStruct((stored.shape[0], stored.shape[1] // 2), jnp.float32)
    return pl.pallas_call(
        roll_kernel,
        grid_spec=pltpu.PrefetchScalarGridSpec(
            num_scalar_prefetch=1,
            grid=(1,),
            in_specs=[pl.BlockSpec(stored.shape, lambda i, s: (0, 0))],
            out_specs=[pl.BlockSpec(half.shape, lambda i, s: (0, 0))] * 2,
        ),
        out_shape=[half, half],
    )(place, stored)


def finish_kernel(place, stored, p0, q0, r0, away, out):
    home = p0[...] + (q0[...] + r0[...])
    ring = jnp.concatenate([home, away[...]], axis=1)
    out[...] = stored[...] - pltpu.roll(ring, place[3], 1)


def finish(place, stored, *pieces):
    return pl.pallas_call(
        finish_kernel,
        grid_spec=pltpu.PrefetchScalarGridSpec(
            num_scalar_prefetch=1,
            grid=(1,),
            in_specs=[pl.BlockSpec(p.shape, lambda i, s: (0, 0)) for p in (stored, *pieces)],
            out_specs=pl.BlockSpec(stored.shape, lambda i, s: (0, 0)),
        ),
        out_shape=jax.ShapeDtypeStruct(stored.shape, jnp.float32),
    )(place, stored, *pieces)


def margin_kernel(place, psi, *refs):
    blocks, (keep, send) = refs[:-2], refs[-2:]
    zl, core = place[0], place[1]
    own = jnp.concatenate([ref[...] for ref in blocks[:5]], axis=0)
    pair = jnp.concatenate([ref[...] for ref in blocks[5:]], axis=0)
    low = jnp.where(zl == 0, own, pair)
    high = jnp.where(zl == 0, pair, own)
    left = jnp.concatenate([low, high], axis=0)
    right = jnp.concatenate([psi[0], psi[1]], axis=1)
    both = dot3(left, right, ((1,), (0,)))
    bands = both.shape[1] // 2
    total = both[:, :bands] + turned(both[:, bands:], blocks[0].shape[0])
    first, second = total[:, : bands // 2], total[:, bands // 2 :]
    keep[...] = jnp.where(core == 0, first, second)
    send[...] = jnp.where(core == 0, second, first)


def margin_of(place, psi, by_half, blocks):
    rows, bands = blocks[0].shape[1], psi.shape[2]
    out = jax.ShapeDtypeStruct((8 * blocks[0].shape[0], bands // 2), jnp.float32)
    whole = [pl.BlockSpec(b.shape, lambda i, s: (0, 0)) for b in blocks]
    index = (lambda i, s: (0, s[0], 0)) if by_half else (lambda i, s: (0, 0, 0))
    return pl.pallas_call(
        margin_kernel,
        grid_spec=pltpu.PrefetchScalarGridSpec(
            num_scalar_prefetch=1,
            grid=(1,),
            in_specs=[pl.BlockSpec((2, rows, bands), index), *whole],
            out_specs=[pl.BlockSpec(out.shape, lambda i, s: (0, 0))] * 2,
        ),
        out_shape=[out, out],
    )(place, psi, *blocks)


def correct_kernel(place, psi, psi_pair, mine, other, p0, p1, p2a, p2b, p3):
    zl, core = place[0], place[1]
    cols = p0.shape[0]

    def weighted(which):
        a = mine[which].reshape(4 * cols, -1)
        b = other[which].reshape(4 * cols, -1)
        return jnp.concatenate([jnp.where(core == 0, a, b), jnp.where(core == 0, b, a)], axis=1)

    w0, w1 = weighted(0), weighted(1)
    own, pair = jnp.where(zl == 0, w0, w1), jnp.where(zl == 0, w1, w0)
    left = jnp.concatenate([own, -turned(own, cols), pair, -turned(pair, cols)], axis=1)
    right = jnp.concatenate([psi[0], psi[1], psi_pair[0], psi_pair[1]], axis=1)
    out = dot3(left, right, ((1,), (1,)))
    p0[...] = out[:cols]
    p1[...] = out[cols : 2 * cols]
    p2a[...] = out[2 * cols : 2 * cols + cols // 2]
    p2b[...] = out[2 * cols + cols // 2 : 3 * cols]
    p3[...] = out[3 * cols :]


def correct_with(place, psi, psi_pair, mine, other, pair):
    _, rows, bands = psi_pair.shape
    cols = mine.shape[2]
    w_spec = pl.BlockSpec(
        (2, 4, cols, bands // 2), lambda i, s: (0, (1 - s[0]) if pair else s[0], 0, 0)
    )
    shapes = [(cols, rows), (cols, rows), (cols // 2, rows), (cols // 2, rows), (cols, rows)]
    return pl.pallas_call(
        correct_kernel,
        grid_spec=pltpu.PrefetchScalarGridSpec(
            num_scalar_prefetch=1,
            grid=(1,),
            in_specs=[
                pl.BlockSpec((2, rows, bands), lambda i, s: (0, s[0], 0)),
                pl.BlockSpec((2, rows, bands), lambda i, s: (0, 0, 0)),
                w_spec,
                w_spec,
            ],
            out_specs=[pl.BlockSpec(s, lambda i, s: (0, 0)) for s in shapes],
        ),
        out_shape=[jax.ShapeDtypeStruct(s, jnp.float32) for s in shapes],
    )(place, psi, psi_pair, mine, other)


def gather_y(block):
    half = block.shape[0] // 2
    before = shifted(block, "y", 1)
    after = shifted(block, "y", -1)
    far_a = shifted(before[:half], "y", 1)
    far_b = shifted(after[half:], "y", -1)
    return [block, after, far_a, far_b, before]


def scatter_y(p0, p1, p2a, p2b, p3):
    half = p2a.shape[0]
    up = shifted(p2a, "y", 1)
    down = shifted(p2b, "y", -1)
    to_next = jnp.concatenate([p1[:half] + up, p1[half:]], 0)
    to_prev = jnp.concatenate([p3[:half], p3[half:] + down], 0)
    return p0, shifted(to_next, "y", 1), shifted(to_prev, "y", -1)


def per_device(psi, dpsi, band_weight, panel_band, slab_offset):
    zl, core = lax.axis_index("zl"), lax.axis_index("c")
    rows, nb = psi.shape[1:]
    half = rows // 2
    np_dev = dpsi.shape[2]
    turn = slab_offset[lax.axis_index(("x", "zh", "c"))] + zl * half
    place = jnp.stack([zl, core, (2 * rows - turn) % rows, turn % rows]).astype(jnp.int32)
    stored = dpsi.swapaxes(1, 2).reshape(2 * np_dev, rows)
    mine, other = roll_out(place, stored)
    pair = shifted(other, "zl", 1)
    psi_other = lax.dynamic_slice_in_dim(psi, (1 - zl) * half, half, 1)
    psi_pair = shifted(psi_other, "zl", 1)
    blocks = gather_y(mine)
    blocks = blocks + gather_y(pair)
    keep_own, send_own = margin_of(place, psi, True, blocks)
    own = keep_own + shifted(send_own, "c", 1)
    keep_pair, send_pair = margin_of(place, psi_pair, False, blocks)
    paired = keep_pair + shifted(send_pair, "c", 1)
    first = zl == 0
    groups = lax.axis_size(SPREAD)
    over_c = jnp.stack([jnp.where(first, own, paired), jnp.where(first, paired, own)])
    over_c = over_c.reshape(groups, 2 * np_dev, nb // 2)
    total = lax.all_to_all(over_c, SPREAD, 0, 0, tiled=True).sum(0)
    weight = lax.dynamic_slice_in_dim(band_weight, panel_band[core] * PANEL, PANEL)
    weighted = total * weight[None, :]
    w_mine = everyone(weighted, SPREAD).reshape(2, groups // 2, 2 * np_dev, nb // 2)
    w_other = shifted(w_mine, "c", 1)
    away = correct_with(place, psi, psi_pair, w_mine, w_other, True)
    b0, b1, b2 = scatter_y(*away)
    away = shifted(b0 + (b1 + b2), "zl", 1)
    home = scatter_y(*correct_with(place, psi, psi_pair, w_mine, w_other, False))
    out = finish(place, stored, *home, away)
    return out.reshape(2, np_dev, rows).swapaxes(1, 2)


def solution(mesh):
    fine = Mesh(mesh.devices.reshape(4, 2, 2, 4, 2), AXES)
    ga, ba = ("x", "zh", "c"), ("y", "zl")
    in_specs = (P(None, ga, ba), P(None, ga, ba), P(), P(ba), P())

    return jax.shard_map(
        per_device, mesh=fine, in_specs=in_specs, out_specs=P(None, ga, ba), check_vma=False
    )
```

```python
import jax
import jax.numpy as jnp
from jax import lax
from jax.experimental import pallas as pl
from jax.experimental.pallas import tpu as pltpu
from jax.sharding import Mesh
from jax.sharding import PartitionSpec as P


PANEL = 128
AXES = ("x", "zh", "c", "y", "zl")
REDUCE = ("x", "zh")
SPREAD = ("zl", "x", "zh")
CHUNKS = 4
F32 = jnp.float32


def shifted(value, axis, step):
    n = lax.axis_size(axis)
    return lax.ppermute(value, axis, [(i, (i + step) % n) for i in range(n)])


def traded(value, axes):
    return lax.all_to_all(value, axes, 0, 0, tiled=True)


def everyone(value, axes):
    return traded(jnp.broadcast_to(value[None], (lax.axis_size(axes), *value.shape)), axes)


def split(value):
    high = value.astype(jnp.bfloat16)
    low = (value - high.astype(F32)).astype(jnp.bfloat16)
    return high, low


def dot3(left, right, dims):
    (lh, ll), (rh, rl) = left, right

    def dot(a, b):
        return lax.dot_general(a, b, (dims, ((), ())), preferred_element_type=F32)

    return dot(lh, rh) + (dot(lh, rl) + dot(ll, rh))


def turned(value, block):
    half = block // 2
    pieces = []
    for k in range(0, value.shape[0], block):
        pieces += [value[k + half : k + block], -value[k : k + half]]
    return jnp.concatenate(pieces, axis=0)


def whole(value):
    zeros = (0,) * value.ndim
    return pl.BlockSpec(value.shape, lambda i, s: zeros)


def call(kernel, place, args, in_specs, out_shapes, flops=0):
    outs = [jax.ShapeDtypeStruct(s, d) for s, d in out_shapes]
    cost = pl.CostEstimate(flops=flops, bytes_accessed=0, transcendentals=0)
    return pl.pallas_call(
        kernel,
        grid_spec=pltpu.PrefetchScalarGridSpec(
            num_scalar_prefetch=1,
            grid=(1,),
            in_specs=in_specs,
            out_specs=[whole(o) for o in outs],
        ),
        out_shape=outs,
        cost_estimate=cost if flops else None,
    )(place, *args)


def roll_kernel(place, stored, mine, other):
    rows = stored.shape[1]
    lined = pltpu.roll(stored[...], place[2], 1)
    mine[...] = lined[:, : rows // 2]
    other[...] = lined[:, rows // 2 :]


def finish_kernel(place, stored, p0, q0, r0, away, out):
    home = p0[...] + (q0[...] + r0[...])
    ring = jnp.concatenate([home, away[...]], axis=1)
    out[...] = stored[...] - pltpu.roll(ring, place[3], 1)


def lined_up(place, blocks):
    own = jnp.concatenate([ref[...] for ref in blocks[:5]], axis=0)
    pair = jnp.concatenate([ref[...] for ref in blocks[5:]], axis=0)
    first = place[0] == 0
    low, high = jnp.where(first, own, pair), jnp.where(first, pair, own)
    return jnp.concatenate([low, high], axis=0)


def put(place, total, cols, keep, send):
    bands = total.shape[1]
    left, right = total[:, : bands // 2], total[:, bands // 2 :]
    first = place[1] == 0
    shards, blocks, rows = keep.shape[:3]
    for ref, value in ((keep, jnp.where(first, left, right)), (send, jnp.where(first, right, left))):
        for b in range(blocks):
            for s in range(shards):
                at = b * cols + s * rows
                ref[s, b] = value[at : at + rows]


def own_kernel(place, psi, *refs):
    blocks, (keep, send) = refs[:-2], refs[-2:]
    cols = blocks[0].shape[0]
    left = split(lined_up(place, blocks))
    right = split(jnp.concatenate([psi[0], psi[1]], axis=1))
    both = dot3(left, right, ((1,), (0,)))
    bands = both.shape[1] // 2
    put(place, both[:, :bands] + turned(both[:, bands:], cols), cols, keep, send)


def pair_kernel(place, re0, re1, im0, *refs):
    blocks, out = refs[:-1], refs[-1]
    cols, part = blocks[0].shape[0], im0.shape[0]
    left = split(lined_up(place, blocks))
    real = split(jnp.concatenate([re0[...], re1[...]], axis=0))
    total = dot3(left, real, ((1,), (0,)))
    left = tuple(v[:, :part] for v in left)
    out[...] = total + turned(dot3(left, split(im0[...]), ((1,), (0,))), cols)


def last_kernel(place, im1, before, *refs):
    blocks, (keep, send) = refs[:-2], refs[-2:]
    cols = blocks[0].shape[0]
    left = split(lined_up(place, blocks))
    total = turned(dot3(left, split(im1[...]), ((1,), (0,))), cols)
    put(place, before[...] + total, cols, keep, send)


def ready_kernel(place, psi, re0, re1, im0, im1, high, low):
    real = jnp.concatenate([re0[...], re1[...]], axis=0)
    imag = jnp.concatenate([im0[...], im1[...]], axis=0)
    value = jnp.concatenate([psi[0], psi[1], real, imag], axis=1)
    high[...], low[...] = split(value)


def weights(place, mine, other, half, r, count):
    def gathered(ref, which):
        v = ref[which]
        shards, rows = v.shape[0], v.shape[-2]
        tiles = [v[s, half, k] for k in range(r, r + count) for s in range(shards)]
        return jnp.concatenate(tiles, axis=0), shards * rows

    first = place[1] == 0
    out = []
    for which in (0, 1):
        a, cols = gathered(mine, which)
        b, _ = gathered(other, which)
        out.append(jnp.concatenate([jnp.where(first, a, b), jnp.where(first, b, a)], axis=1))
    zero = place[0] == 0
    own, pair = jnp.where(zero, out[0], out[1]), jnp.where(zero, out[1], out[0])
    return jnp.concatenate([own, -turned(own, cols), pair, -turned(pair, cols)], axis=1)


def far_kernel(place, high, low, mine, other, to_a, to_b):
    left = split(weights(place, mine, other, 0, 0, 1))
    out = dot3(left, (high[...], low[...]), ((1,), (1,)))
    half = out.shape[0] // 2
    to_a[...], to_b[...] = out[:half], out[half:]


def near_kernel(place, high, low, mine, other, up, down, p0, to_next, to_prev):
    left = split(weights(place, mine, other, 0, 0, 3))
    out = dot3(left, (high[...], low[...]), ((1,), (1,)))
    cols = p0.shape[0]
    half = cols // 2
    p0[...] = out[:cols]
    to_next[:half] = out[cols : cols + half] + up[...]
    to_next[half:] = out[cols + half : 2 * cols]
    to_prev[:half] = out[2 * cols : 2 * cols + half]
    to_prev[half:] = out[2 * cols + half :] + down[...]


def gather_y(block):
    half = block.shape[0] // 2
    before = shifted(block, "y", 1)
    after = shifted(block, "y", -1)
    far_a = shifted(before[:half], "y", 1)
    far_b = shifted(after[half:], "y", -1)
    return [block, after, far_a, far_b, before]


def per_device(psi, dpsi, band_weight, panel_band, slab_offset):
    zl, core = lax.axis_index("zl"), lax.axis_index("c")
    rows, nb = psi.shape[1:]
    half, cols = rows // 2, 2 * dpsi.shape[2]
    part = 2 * half // CHUNKS
    turn = slab_offset[lax.axis_index(("x", "zh", "c"))] + zl * half
    place = jnp.stack([zl, core, (2 * rows - turn) % rows, turn % rows]).astype(jnp.int32)
    stored = dpsi.swapaxes(1, 2).reshape(cols, rows)
    psi_spec = pl.BlockSpec((2, half, nb), lambda i, s: (0, s[0], 0))

    pieces = []
    for k in range(CHUNKS):
        plane, at = divmod(k * part, half)
        start = (plane, (1 - zl) * half + at, 0)
        piece = lax.dynamic_slice(psi, start, (1, part, nb))[0]
        pieces.append(shifted(piece, "zl", 1))
    mine, other = call(roll_kernel, place, [stored], [whole(stored)], [((cols, half), F32)] * 2)
    pair = shifted(other, "zl", 1)
    blocks = gather_y(mine) + gather_y(pair)

    shards = lax.axis_size(REDUCE)
    mac = 6 * 8 * cols * half
    out = [((shards, 8, cols // shards, nb // 2), F32)] * 2
    specs = [whole(b) for b in blocks]
    keep, send = call(own_kernel, place, [psi, *blocks], [psi_spec, *specs], out, mac * 2 * nb)
    over_c = keep + shifted(send, "c", 1)
    own_sum = traded(over_c, REDUCE).sum(0)

    early = pieces[:3]
    partial = call(
        pair_kernel,
        place,
        [*early, *blocks],
        [*map(whole, early), *specs],
        [((8 * cols, nb), F32)],
        mac * nb * 3 // 2,
    )[0]
    late = [pl.BlockSpec((b.shape[0], part), lambda i, s: (0, 1)) for b in blocks]
    keep, send = call(
        last_kernel,
        place,
        [pieces[3], partial, *blocks],
        [whole(pieces[3]), whole(partial), *late],
        out,
        mac * nb // 2,
    )
    over_c = keep + shifted(send, "c", 1)
    pair_sum = traded(over_c, REDUCE).sum(0)
    total = own_sum + shifted(pair_sum, "zl", 1)
    weight = lax.dynamic_slice_in_dim(band_weight, panel_band[core] * PANEL, PANEL)
    weighted = (total * weight).reshape(2, 4, cols // shards, nb // 2)

    high, low = call(
        ready_kernel,
        place,
        [psi, *pieces],
        [psi_spec, *map(whole, pieces)],
        [((half, 4 * nb), jnp.bfloat16)] * 2,
        mac,
    )
    far = weighted[:, 2:3]
    near = jnp.concatenate([weighted[:, :2], weighted[:, 3:]], axis=1)
    far_mine = everyone(far, SPREAD)
    far_mine = far_mine.reshape(2, shards, *far.shape)
    far_other = shifted(far_mine, "c", 1)
    near_mine = everyone(near, SPREAD)
    near_mine = near_mine.reshape(2, shards, *near.shape)
    near_other = shifted(near_mine, "c", 1)

    def of_half(value, which):
        def index(i, s):
            return (0, 0, 1 - s[0] if which else s[0], 0, 0, 0)

        return pl.BlockSpec((2, shards, 1, *value.shape[3:]), index)

    steps = []
    for which in (1, 0):
        args = [high, low, far_mine, far_other]
        specs = [whole(high), whole(low), *[of_half(far_mine, which)] * 2]
        shapes = [((cols // 2, half), F32)] * 2
        a, b = call(far_kernel, place, args, specs, shapes, mac * nb // 2)
        steps.append((shifted(a, "y", 1), shifted(b, "y", -1)))
    results = []
    for which in (1, 0):
        up, down = steps[1 - which]
        args = [high, low, near_mine, near_other, up, down]
        specs = [whole(high), whole(low), *[of_half(near_mine, which)] * 2, whole(up), whole(down)]
        shapes = [((cols, half), F32)] * 3
        p0, to_next, to_prev = call(near_kernel, place, args, specs, shapes, mac * nb * 3 // 2)
        q0 = shifted(to_next, "y", 1)
        r0 = shifted(to_prev, "y", -1)
        results.append((p0, q0, r0))
    p0, q0, r0 = results[0]
    away = shifted(p0 + (q0 + r0), "zl", 1)
    args = [stored, *results[1], away]
    done = call(finish_kernel, place, args, [whole(a) for a in args], [(stored.shape, F32)])[0]
    return done.reshape(2, cols // 2, rows).swapaxes(1, 2)


def solution(mesh):
    fine = Mesh(mesh.devices.reshape(4, 2, 2, 4, 2), AXES)
    ga, ba = ("x", "zh", "c"), ("y", "zl")
    in_specs = (P(None, ga, ba), P(None, ga, ba), P(), P(ba), P())

    return jax.shard_map(
        per_device, mesh=fine, in_specs=in_specs, out_specs=P(None, ga, ba), check_vma=False
    )
```

```python
import jax
import jax.numpy as jnp
from jax import lax
from jax.experimental import pallas as pl
from jax.experimental.pallas import tpu as pltpu
from jax.sharding import Mesh
from jax.sharding import PartitionSpec as P


PANEL = 128
LANES = 128
AXES = ("x", "zh", "c", "y", "zl")
REDUCE = ("x", "zh")
SPREAD = ("zl", "x", "zh")
CHUNKS = 4
F32 = jnp.float32


def shifted(value, axis, step):
    n = lax.axis_size(axis)
    return lax.ppermute(value, axis, [(i, (i + step) % n) for i in range(n)])


def traded(value, axes):
    return lax.all_to_all(value, axes, 0, 0, tiled=True)


def everyone(value, axes):
    return traded(jnp.broadcast_to(value[None], (lax.axis_size(axes), *value.shape)), axes)


def split(value):
    high = value.astype(jnp.bfloat16)
    low = (value - high.astype(F32)).astype(jnp.bfloat16)
    return high, low


def dot3(left, right, dims):
    (lh, ll), (rh, rl) = left, right

    def dot(a, b):
        return lax.dot_general(a, b, (dims, ((), ())), preferred_element_type=F32)

    return dot(lh, rh) + (dot(lh, rl) + dot(ll, rh))


def turned(value, block):
    half = block // 2
    pieces = []
    for k in range(0, value.shape[0], block):
        pieces += [value[k + half : k + block], -value[k : k + half]]
    return jnp.concatenate(pieces, axis=0)


def whole(value):
    zeros = (0,) * value.ndim
    return pl.BlockSpec(value.shape, lambda i, s: zeros)


def call(kernel, place, args, in_specs, out_shapes, flops=0, scratch=()):
    outs = [jax.ShapeDtypeStruct(s, d) for s, d in out_shapes]
    cost = pl.CostEstimate(flops=flops, bytes_accessed=0, transcendentals=0)
    return pl.pallas_call(
        kernel,
        grid_spec=pltpu.PrefetchScalarGridSpec(
            num_scalar_prefetch=1,
            grid=(1,),
            in_specs=in_specs,
            out_specs=[whole(o) for o in outs],
            scratch_shapes=list(scratch),
        ),
        out_shape=outs,
        cost_estimate=cost if flops else None,
    )(place, *args)


def rolled(place, which, ring, out):
    turn = place[which]
    tile = turn // LANES
    rest = turn % LANES
    lane = lax.broadcasted_iota(jnp.int32, (ring.shape[0], LANES), 1)

    def load(k):
        at = pl.multiple_of((tile + k) * LANES, LANES)
        return pltpu.roll(ring[:, pl.ds(at, LANES)], (LANES - rest) % LANES, 1)

    now = load(0)
    for k in range(ring.shape[1] // 2 // LANES):
        after = load(k + 1)
        out(k, jnp.where(lane < LANES - rest, now, after))
        now = after


def roll_kernel(place, stored, mine, other, ring):
    rows = stored.shape[1]
    ring[:, :rows] = stored[...]
    ring[:, rows : 2 * rows] = stored[...]
    tiles = rows // 2 // LANES

    def out(k, value):
        ref = mine if k < tiles else other
        at = k % tiles * LANES
        ref[:, at : at + LANES] = value

    rolled(place, 3, ring, out)


def finish_kernel(place, stored, p0, q0, r0, away, out, ring):
    half = away.shape[1]
    home = p0[...] + (q0[...] + r0[...])
    for k in (0, 2):
        ring[:, k * half : (k + 1) * half] = home
        ring[:, (k + 1) * half : (k + 2) * half] = away[...]

    def put(k, value):
        at = slice(k * LANES, (k + 1) * LANES)
        out[:, at] = stored[:, at] - value

    rolled(place, 2, ring, put)


def ready_own(place, psi, high, low):
    bands = psi.shape[2]
    for p in (0, 1):
        h, l = split(psi[p])
        high[:, p * bands : (p + 1) * bands] = h
        low[:, p * bands : (p + 1) * bands] = l


def ready_pair(place, re0, re1, im0, im1, high, low):
    part, bands = re0.shape
    for k, ref in enumerate((re0, re1, im0, im1)):
        h, l = split(ref[...])
        rows = slice(k % 2 * part, (k % 2 + 1) * part)
        high[rows, k // 2 * bands : (k // 2 + 1) * bands] = h
        low[rows, k // 2 * bands : (k // 2 + 1) * bands] = l


def put(place, total, cols, first, keep, send):
    bands = total.shape[1]
    left, right = total[:, : bands // 2], total[:, bands // 2 :]
    south = place[1] == 0
    shards, rows = keep.shape[0], keep.shape[2]
    for ref, value in ((keep, jnp.where(south, left, right)), (send, jnp.where(south, right, left))):
        for b in range(total.shape[0] // cols):
            for s in range(shards):
                at = b * cols + s * rows
                ref[s, first + b] = value[at : at + rows]


def own_kernel(place, psi_high, psi_low, *refs):
    blocks, (high, low, keep, send) = refs[:-4], refs[-4:]
    cols = blocks[0].shape[0]
    for group in (0, 1):
        base = (place[0] if group == 0 else 1 - place[0]) * (4 * cols)
        at = 0
        for ref in blocks[5 * group : 5 * group + 5]:
            h, l = split(ref[...])
            rows = pl.ds(pl.multiple_of(base + at, cols // 2), ref.shape[0])
            high[rows, :] = h
            low[rows, :] = l
            at += ref.shape[0]
    right = (psi_high[...], psi_low[...])
    step = 4 * cols
    bands = psi_high.shape[1] // 2
    for k in (0, 1):
        rows = slice(k * step, (k + 1) * step)
        both = dot3((high[rows], low[rows]), right, ((1,), (0,)))
        total = both[:, :bands] + turned(both[:, bands:], cols)
        put(place, total, cols, 4 * k, keep, send)


def pair_kernel(place, high, low, re0, re1, im0, out):
    part = im0.shape[0]
    cols = out.shape[0] // 8
    real = split(jnp.concatenate([re0[...], re1[...]], axis=0))
    imag = split(im0[...])
    step = 4 * cols
    for k in (0, 1):
        rows = slice(k * step, (k + 1) * step)
        total = dot3((high[rows], low[rows]), real, ((1,), (0,)))
        more = dot3((high[rows, :part], low[rows, :part]), imag, ((1,), (0,)))
        out[rows] = total + turned(more, cols)


def last_kernel(place, high, low, im1, before, keep, send):
    cols = before.shape[0] // 8
    imag = split(im1[...])
    step = 4 * cols
    for k in (0, 1):
        rows = slice(k * step, (k + 1) * step)
        more = dot3((high[rows], low[rows]), imag, ((1,), (0,)))
        put(place, before[rows] + turned(more, cols), cols, 4 * k, keep, send)


def set_weights(place, ref, other, half, base, w_high, w_low):
    zl, core = place[0], place[1]
    _, shards, _, blocks, rows, bands = ref.shape
    cols = shards * rows
    middle = cols // 2
    for which in (0, 1):
        offset = jnp.where(zl == which, 0, 4 * bands)
        for source, spot in ((ref, core), (other, 1 - core)):
            plain = pl.ds(pl.multiple_of(offset + spot * bands, bands), bands)
            cross = pl.ds(pl.multiple_of(offset + (2 + spot) * bands, bands), bands)
            for k in range(blocks):
                for s in range(shards):
                    h, l = split(source[which, s, half, k])
                    at = k * cols + s * rows
                    w_high[pl.ds(pl.multiple_of(base + at, rows), rows), plain] = h
                    w_low[pl.ds(pl.multiple_of(base + at, rows), rows), plain] = l
                    if s * rows < middle:
                        at += middle
                    else:
                        at, h, l = at - middle, -h, -l
                    w_high[pl.ds(pl.multiple_of(base + at, rows), rows), cross] = h
                    w_low[pl.ds(pl.multiple_of(base + at, rows), rows), cross] = l


def product(own_h, own_l, pair_h, pair_l, w_high, w_low, done):
    bands = own_h.shape[1]
    step = own_h.shape[0] // 2
    dims = ((1,), (1,))
    for k in (0, 1):
        rows = slice(k * step, (k + 1) * step)
        out = dot3((own_h[rows], own_l[rows]), (w_high[:, :bands], w_low[:, :bands]), dims)
        out += dot3((pair_h[rows], pair_l[rows]), (w_high[:, bands:], w_low[:, bands:]), dims)
        done(rows, out.T)


def far_kernel(place, oh, ol, ph, pl_, mine, other, pair_a, pair_b, own_a, own_b, w_high, w_low):
    cols = w_high.shape[0] // 2
    half = cols // 2
    for k in (0, 1):
        base = jnp.where(place[0] == k, cols, 0)
        set_weights(place, mine, other, k, base, w_high, w_low)

    def done(rows, out):
        for k, ref in enumerate((pair_a, pair_b, own_a, own_b)):
            ref[:, rows] = out[k * half : (k + 1) * half]

    product(oh, ol, ph, pl_, w_high, w_low, done)


def near_kernel(place, oh, ol, ph, pl_, mine, other, up, down, p0, to_next, to_prev, w_high, w_low):
    cols = p0.shape[0]
    half = cols // 2
    set_weights(place, mine, other, 0, 0, w_high, w_low)

    def done(rows, out):
        p0[:, rows] = out[:cols]
        to_next[:half, rows] = out[cols : cols + half] + up[:, rows]
        to_next[half:, rows] = out[cols + half : 2 * cols]
        to_prev[:half, rows] = out[2 * cols : 2 * cols + half]
        to_prev[half:, rows] = out[2 * cols + half :] + down[:, rows]

    product(oh, ol, ph, pl_, w_high, w_low, done)


def gather_y(block):
    half = block.shape[0] // 2
    before = shifted(block, "y", 1)
    after = shifted(block, "y", -1)
    far_a = shifted(before[:half], "y", 1)
    far_b = shifted(after[half:], "y", -1)
    return [block, after, far_a, far_b, before]


def per_device(psi, dpsi, band_weight, panel_band, slab_offset):
    zl, core = lax.axis_index("zl"), lax.axis_index("c")
    rows, nb = psi.shape[1:]
    half, cols = rows // 2, 2 * dpsi.shape[2]
    part = 2 * half // CHUNKS
    turn = slab_offset[lax.axis_index(("x", "zh", "c"))] + zl * half
    place = jnp.stack([zl, core, (2 * rows - turn) % rows, turn % rows]).astype(jnp.int32)
    stored = dpsi.swapaxes(1, 2).reshape(cols, rows)
    psi_spec = pl.BlockSpec((2, half, nb), lambda i, s: (0, s[0], 0))

    ring = [pltpu.VMEM((cols, 2 * rows + LANES), F32)]
    mine, other = call(
        roll_kernel, place, [stored], [whole(stored)], [((cols, half), F32)] * 2, scratch=ring
    )
    pair = shifted(other, "zl", 1)
    pieces = []
    for k in range(CHUNKS):
        plane, at = divmod(k * part, half)
        start = (plane, (1 - zl) * half + at, 0)
        piece = lax.dynamic_slice(psi, start, (1, part, nb))[0]
        pieces.append(shifted(piece, "zl", 1))
    blocks = gather_y(mine) + gather_y(pair)

    mac = 6 * 8 * cols * half
    b16 = [((half, 2 * nb), jnp.bfloat16)] * 2
    psi_own = call(ready_own, place, [psi], [psi_spec], b16, mac)
    shards = lax.axis_size(REDUCE)
    out = [((shards, 8, cols // shards, nb // 2), F32)] * 2
    args = [*psi_own, *blocks]
    shapes = [((8 * cols, half), jnp.bfloat16)] * 2 + out
    high, low, keep, send = call(own_kernel, place, args, [*map(whole, args)], shapes, mac * 2 * nb)
    over_c = keep + shifted(send, "c", 1)
    own_sum = traded(over_c, REDUCE).sum(0)

    args = [high, low, *pieces[:3]]
    shapes = [((8 * cols, nb), F32)]
    partial = call(pair_kernel, place, args, [*map(whole, args)], shapes, mac * nb * 3 // 2)[0]
    late = pl.BlockSpec((8 * cols, part), lambda i, s: (0, 1))
    args = [high, low, pieces[3], partial]
    specs = [late, late, whole(pieces[3]), whole(partial)]
    keep, send = call(last_kernel, place, args, specs, out, mac * nb // 2)
    over_c = keep + shifted(send, "c", 1)
    pair_sum = traded(over_c, REDUCE).sum(0)
    total = own_sum + shifted(pair_sum, "zl", 1)
    weight = lax.dynamic_slice_in_dim(band_weight, panel_band[core] * PANEL, PANEL)
    weighted = (total * weight).reshape(2, 4, cols // shards, nb // 2)

    psi_pair = call(ready_pair, place, pieces, [*map(whole, pieces)], b16, mac)
    far = weighted[:, 2:3]
    near = jnp.concatenate([weighted[:, :2], weighted[:, 3:]], axis=1)
    far_mine = everyone(far, SPREAD)
    far_mine = far_mine.reshape(2, shards, *far.shape)
    far_other = shifted(far_mine, "c", 1)
    near_mine = everyone(near, SPREAD)
    near_mine = near_mine.reshape(2, shards, *near.shape)
    near_other = shifted(near_mine, "c", 1)

    waves = [*psi_own, *psi_pair]
    args = [*waves, far_mine, far_other]
    shapes = [((cols // 2, half), F32)] * 4
    room = [pltpu.VMEM((2 * cols, 4 * nb), jnp.bfloat16)] * 2
    pa, pb, oa, ob = call(far_kernel, place, args, [*map(whole, args)], shapes, mac * nb, room)
    steps = [
        (shifted(pa, "y", 1), shifted(pb, "y", -1)), (shifted(oa, "y", 1), shifted(ob, "y", -1))
    ]
    results = []
    room = [pltpu.VMEM((3 * cols, 4 * nb), jnp.bfloat16)] * 2
    for which in (1, 0):
        up, down = steps[1 - which]
        args = [*waves, near_mine, near_other, up, down]

        def index(i, s, which=which):
            return (0, 0, 1 - s[0] if which else s[0], 0, 0, 0)

        near_spec = pl.BlockSpec((2, shards, 1, *near.shape[1:]), index)
        specs = [*map(whole, waves), near_spec, near_spec, whole(up), whole(down)]
        shapes = [((cols, half), F32)] * 3
        p0, to_next, to_prev = call(
            near_kernel, place, args, specs, shapes, mac * nb * 3 // 2, room
        )
        q0 = shifted(to_next, "y", 1)
        r0 = shifted(to_prev, "y", -1)
        results.append((p0, q0, r0))
    p0, q0, r0 = results[0]
    away = shifted(p0 + (q0 + r0), "zl", 1)
    args = [stored, *results[1], away]
    done = call(
        finish_kernel, place, args, [*map(whole, args)], [(stored.shape, F32)], scratch=ring
    )[0]
    return done.reshape(2, cols // 2, rows).swapaxes(1, 2)


def solution(mesh):
    fine = Mesh(mesh.devices.reshape(4, 2, 2, 4, 2), AXES)
    ga, ba = ("x", "zh", "c"), ("y", "zl")
    in_specs = (P(None, ga, ba), P(None, ga, ba), P(), P(ba), P())

    return jax.shard_map(
        per_device, mesh=fine, in_specs=in_specs, out_specs=P(None, ga, ba), check_vma=False
    )
```

```python
from functools import partial as partial_of

import jax
import jax.numpy as jnp
from jax import lax
from jax.experimental import pallas as pl
from jax.experimental.pallas import tpu as pltpu
from jax.sharding import Mesh
from jax.sharding import PartitionSpec as P


PANEL = 128
LANES = 128
AXES = ("x", "zh", "c", "y", "zl")
REDUCE = ("x", "zh")
SPREAD = ("zl", "x", "zh")
CHUNKS = 4
F32 = jnp.float32


def shifted(value, axis, step):
    n = lax.axis_size(axis)
    return lax.ppermute(value, axis, [(i, (i + step) % n) for i in range(n)])


def traded(value, axes):
    return lax.all_to_all(value, axes, 0, 0, tiled=True)


def everyone(value, axes):
    return traded(jnp.broadcast_to(value[None], (lax.axis_size(axes), *value.shape)), axes)


def split(value):
    high = value.astype(jnp.bfloat16)
    low = (value - high.astype(F32)).astype(jnp.bfloat16)
    return high, low


def dot3(left, right, dims):
    (lh, ll), (rh, rl) = left, right

    def dot(a, b):
        return lax.dot_general(a, b, (dims, ((), ())), preferred_element_type=F32)

    return dot(lh, rh) + (dot(lh, rl) + dot(ll, rh))


def turned(value, block):
    half = block // 2
    pieces = []
    for k in range(0, value.shape[0], block):
        pieces += [value[k + half : k + block], -value[k : k + half]]
    return jnp.concatenate(pieces, axis=0)


def call(kernel, place, args, out_shapes, flops=0, scratch=(), limit=8):
    outs = [jax.ShapeDtypeStruct(s, d) for s, d in out_shapes]
    cost = pl.CostEstimate(flops=flops, bytes_accessed=0, transcendentals=0)
    vmem = pl.BlockSpec(memory_space=pltpu.VMEM)
    return pl.pallas_call(
        kernel,
        in_specs=[pl.BlockSpec(memory_space=pltpu.SMEM)] + [vmem] * len(args),
        out_specs=[vmem] * len(outs),
        out_shape=outs,
        scratch_shapes=list(scratch),
        cost_estimate=cost if flops else None,
        compiler_params=pltpu.CompilerParams(vmem_limit_bytes=limit * 2**20),
    )(place, *args)


def rolled(place, which, ring, out):
    turn = place[which]
    tile = turn // LANES
    rest = turn % LANES
    lane = lax.broadcasted_iota(jnp.int32, (ring.shape[0], LANES), 1)

    def load(k):
        at = pl.multiple_of((tile + k) * LANES, LANES)
        return pltpu.roll(ring[:, pl.ds(at, LANES)], (LANES - rest) % LANES, 1)

    now = load(0)
    for k in range(ring.shape[1] // 2 // LANES):
        after = load(k + 1)
        out(k, jnp.where(lane < LANES - rest, now, after))
        now = after


def roll_kernel(place, stored, mine, other, ring):
    rows = stored.shape[1]
    ring[:, :rows] = stored[...]
    ring[:, rows : 2 * rows] = stored[...]
    tiles = rows // 2 // LANES

    def out(k, value):
        ref = mine if k < tiles else other
        at = k % tiles * LANES
        ref[:, at : at + LANES] = value

    rolled(place, 3, ring, out)


def finish_kernel(place, stored, p0, q0, r0, away, out, ring):
    half = away.shape[1]
    home = p0[...] + (q0[...] + r0[...])
    for k in (0, 2):
        ring[:, k * half : (k + 1) * half] = home
        ring[:, (k + 1) * half : (k + 2) * half] = away[...]

    def put(k, value):
        at = slice(k * LANES, (k + 1) * LANES)
        out[:, at] = stored[:, at] - value

    rolled(place, 2, ring, put)


def ready_own(place, psi, high, low):
    rows, bands = high.shape[0], psi.shape[2]
    at = pl.multiple_of(place[0] * rows, rows)
    for p in (0, 1):
        h, l = split(psi[p, pl.ds(at, rows), :])
        high[:, p * bands : (p + 1) * bands] = h
        low[:, p * bands : (p + 1) * bands] = l


def ready_pair(place, re0, re1, im0, im1, high, low):
    part, bands = re0.shape
    for k, ref in enumerate((re0, re1, im0, im1)):
        h, l = split(ref[...])
        rows = slice(k % 2 * part, (k % 2 + 1) * part)
        high[rows, k // 2 * bands : (k // 2 + 1) * bands] = h
        low[rows, k // 2 * bands : (k // 2 + 1) * bands] = l


def put(place, total, cols, first, keep, send):
    bands = total.shape[1]
    left, right = total[:, : bands // 2], total[:, bands // 2 :]
    south = place[1] == 0
    shards, rows = keep.shape[0], keep.shape[2]
    for ref, value in ((keep, jnp.where(south, left, right)), (send, jnp.where(south, right, left))):
        for b in range(total.shape[0] // cols):
            for s in range(shards):
                at = b * cols + s * rows
                ref[s, first + b] = value[at : at + rows]


def own_kernel(place, psi_high, psi_low, *refs):
    blocks, (high, low, keep, send) = refs[:-4], refs[-4:]
    cols = blocks[0].shape[0]
    for group in (0, 1):
        base = (place[0] if group == 0 else 1 - place[0]) * (4 * cols)
        at = 0
        for ref in blocks[5 * group : 5 * group + 5]:
            h, l = split(ref[...])
            rows = pl.ds(pl.multiple_of(base + at, cols // 2), ref.shape[0])
            high[rows, :] = h
            low[rows, :] = l
            at += ref.shape[0]
    right = (psi_high[...], psi_low[...])
    step = 4 * cols
    bands = psi_high.shape[1] // 2
    for k in (0, 1):
        rows = slice(k * step, (k + 1) * step)
        both = dot3((high[rows], low[rows]), right, ((1,), (0,)))
        total = both[:, :bands] + turned(both[:, bands:], cols)
        put(place, total, cols, 4 * k, keep, send)


def pair_kernel(place, high, low, re0, re1, im0, out):
    part = im0.shape[0]
    cols = out.shape[0] // 8
    real = split(jnp.concatenate([re0[...], re1[...]], axis=0))
    imag = split(im0[...])
    step = 4 * cols
    for k in (0, 1):
        rows = slice(k * step, (k + 1) * step)
        total = dot3((high[rows], low[rows]), real, ((1,), (0,)))
        more = dot3((high[rows, :part], low[rows, :part]), imag, ((1,), (0,)))
        out[rows] = total + turned(more, cols)


def last_kernel(place, high, low, im1, before, keep, send):
    cols, part = before.shape[0] // 8, im1.shape[0]
    imag = split(im1[...])
    step = 4 * cols
    for k in (0, 1):
        rows = slice(k * step, (k + 1) * step)
        more = dot3((high[rows, part:], low[rows, part:]), imag, ((1,), (0,)))
        put(place, before[rows] + turned(more, cols), cols, 4 * k, keep, send)


def set_weights(place, ref, other, half, base, w_high, w_low):
    zl, core = place[0], place[1]
    _, shards, _, blocks, rows, bands = ref.shape
    cols = shards * rows
    middle = cols // 2
    for which in (0, 1):
        offset = jnp.where(zl == which, 0, 4 * bands)
        for source, spot in ((ref, core), (other, 1 - core)):
            plain = pl.ds(pl.multiple_of(offset + spot * bands, bands), bands)
            cross = pl.ds(pl.multiple_of(offset + (2 + spot) * bands, bands), bands)
            for k in range(blocks):
                for s in range(shards):
                    h, l = split(source[which, s, half, k])
                    at = k * cols + s * rows
                    w_high[pl.ds(pl.multiple_of(base + at, rows), rows), plain] = h
                    w_low[pl.ds(pl.multiple_of(base + at, rows), rows), plain] = l
                    if s * rows < middle:
                        at += middle
                    else:
                        at, h, l = at - middle, -h, -l
                    w_high[pl.ds(pl.multiple_of(base + at, rows), rows), cross] = h
                    w_low[pl.ds(pl.multiple_of(base + at, rows), rows), cross] = l


def product(own_h, own_l, pair_h, pair_l, w_high, w_low, done):
    bands = own_h.shape[1]
    step = own_h.shape[0] // 2
    dims = ((1,), (1,))
    for k in (0, 1):
        rows = slice(k * step, (k + 1) * step)
        out = dot3((own_h[rows], own_l[rows]), (w_high[:, :bands], w_low[:, :bands]), dims)
        out += dot3((pair_h[rows], pair_l[rows]), (w_high[:, bands:], w_low[:, bands:]), dims)
        done(rows, out.T)


def far_kernel(place, oh, ol, ph, pl_, mine, other, pair_a, pair_b, own_a, own_b, w_high, w_low):
    cols = w_high.shape[0] // 2
    half = cols // 2
    for k in (0, 1):
        base = jnp.where(place[0] == k, cols, 0)
        set_weights(place, mine, other, k, base, w_high, w_low)

    def done(rows, out):
        for k, ref in enumerate((pair_a, pair_b, own_a, own_b)):
            ref[:, rows] = out[k * half : (k + 1) * half]

    product(oh, ol, ph, pl_, w_high, w_low, done)


def near_kernel(which, place, oh, ol, ph, pl_, mine, other, up, down, p0, to_next, to_prev, w_high, w_low):
    cols = p0.shape[0]
    half = cols // 2
    column_half = 1 - place[0] if which else place[0]
    set_weights(place, mine, other, column_half, 0, w_high, w_low)

    def done(rows, out):
        p0[:, rows] = out[:cols]
        to_next[:half, rows] = out[cols : cols + half] + up[:, rows]
        to_next[half:, rows] = out[cols + half : 2 * cols]
        to_prev[:half, rows] = out[2 * cols : 2 * cols + half]
        to_prev[half:, rows] = out[2 * cols + half :] + down[:, rows]

    product(oh, ol, ph, pl_, w_high, w_low, done)


def gather_y(block):
    half = block.shape[0] // 2
    before = shifted(block, "y", 1)
    after = shifted(block, "y", -1)
    far_a = shifted(before[:half], "y", 1)
    far_b = shifted(after[half:], "y", -1)
    return [block, after, far_a, far_b, before]


def per_device(psi, dpsi, band_weight, panel_band, slab_offset):
    zl, core = lax.axis_index("zl"), lax.axis_index("c")
    rows, nb = psi.shape[1:]
    half, cols = rows // 2, 2 * dpsi.shape[2]
    part = 2 * half // CHUNKS
    turn = slab_offset[lax.axis_index(("x", "zh", "c"))] + zl * half
    place = jnp.stack([zl, core, (2 * rows - turn) % rows, turn % rows]).astype(jnp.int32)
    stored = dpsi.swapaxes(1, 2).reshape(cols, rows)

    ring = [pltpu.VMEM((cols, 2 * rows + LANES), F32)]
    mine, other = call(
        roll_kernel, place, [stored], [((cols, half), F32)] * 2, scratch=ring
    )
    pair = shifted(other, "zl", 1)
    pieces = []
    for k in range(CHUNKS):
        plane, at = divmod(k * part, half)
        start = (plane, (1 - zl) * half + at, 0)
        piece = lax.dynamic_slice(psi, start, (1, part, nb))[0]
        pieces.append(shifted(piece, "zl", 1))
    blocks = gather_y(mine) + gather_y(pair)

    mac = 6 * 8 * cols * half
    b16 = [((half, 2 * nb), jnp.bfloat16)] * 2
    psi_own = call(ready_own, place, [psi], b16, mac)
    shards = lax.axis_size(REDUCE)
    out = [((shards, 8, cols // shards, nb // 2), F32)] * 2
    args = [*psi_own, *blocks]
    shapes = [((8 * cols, half), jnp.bfloat16)] * 2 + out
    high, low, keep, send = call(own_kernel, place, args, shapes, mac * 2 * nb)
    over_c = keep + shifted(send, "c", 1)
    own_sum = traded(over_c, REDUCE).sum(0)

    args = [high, low, *pieces[:3]]
    shapes = [((8 * cols, nb), F32)]
    partial = call(pair_kernel, place, args, shapes, mac * nb * 3 // 2)[0]
    args = [high, low, pieces[3], partial]
    keep, send = call(last_kernel, place, args, out, mac * nb // 2)
    over_c = keep + shifted(send, "c", 1)
    pair_sum = traded(over_c, REDUCE).sum(0)
    total = own_sum + shifted(pair_sum, "zl", 1)
    weight = lax.dynamic_slice_in_dim(band_weight, panel_band[core] * PANEL, PANEL)
    weighted = (total * weight).reshape(2, 4, cols // shards, nb // 2)

    psi_pair = call(ready_pair, place, pieces, b16, mac)
    far = weighted[:, 2:3]
    near = jnp.concatenate([weighted[:, :2], weighted[:, 3:]], axis=1)
    far_mine = everyone(far, SPREAD)
    far_mine = far_mine.reshape(2, shards, *far.shape)
    far_other = shifted(far_mine, "c", 1)
    near_mine = everyone(near, SPREAD)
    near_mine = near_mine.reshape(2, shards, *near.shape)
    near_other = shifted(near_mine, "c", 1)

    waves = [*psi_own, *psi_pair]
    args = [*waves, far_mine, far_other]
    shapes = [((cols // 2, half), F32)] * 4
    room = [pltpu.VMEM((2 * cols, 4 * nb), jnp.bfloat16)] * 2
    pa, pb, oa, ob = call(far_kernel, place, args, shapes, mac * nb, room)
    steps = [
        (shifted(pa, "y", 1), shifted(pb, "y", -1)), (shifted(oa, "y", 1), shifted(ob, "y", -1))
    ]
    results = []
    room = [pltpu.VMEM((3 * cols, 4 * nb), jnp.bfloat16)] * 2
    for which in (1, 0):
        up, down = steps[1 - which]
        args = [*waves, near_mine, near_other, up, down]
        shapes = [((cols, half), F32)] * 3
        p0, to_next, to_prev = call(
            partial_of(near_kernel, which), place, args, shapes, mac * nb * 3 // 2, room
        )
        q0 = shifted(to_next, "y", 1)
        r0 = shifted(to_prev, "y", -1)
        results.append((p0, q0, r0))
    p0, q0, r0 = results[0]
    away = shifted(p0 + (q0 + r0), "zl", 1)
    args = [stored, *results[1], away]
    done = call(
        finish_kernel, place, args, [(stored.shape, F32)], scratch=ring
    )[0]
    return done.reshape(2, cols // 2, rows).swapaxes(1, 2)


def solution(mesh):
    fine = Mesh(mesh.devices.reshape(4, 2, 2, 4, 2), AXES)
    ga, ba = ("x", "zh", "c"), ("y", "zl")
    in_specs = (P(None, ga, ba), P(None, ga, ba), P(), P(ba), P())

    return jax.shard_map(
        per_device, mesh=fine, in_specs=in_specs, out_specs=P(None, ga, ba), check_vma=False
    )
```
